32 devices in a mesh: span: 4 (over y, x), heads: 8 (over z, core).
Axes of the slice: x: 2, y: 2, z: 4, core: 2. Of those that a mesh axis runs over, the one named last changes fastest.
Arguments:
- latents: bfloat16 [4, 6144, 512], P(None, ('span', 'heads')), may hold values from -6 to 6
- rotary_rows: bfloat16 [4, 6144, 64], P(None, ('span', 'heads')), may hold values from -6 to 6
- latent_gain: float32 [512], replicated, may hold values from 0.25 to 1.75
- key_up: bfloat16 [512, 16, 128], P(None, 'heads'), may hold values from -0.25 to 0.25
- value_up: bfloat16 [512, 16, 128], P(None, 'heads'), may hold values from -0.25 to 0.25
Outputs:
- stored_keys: bfloat16 [4, 6144, 16, 192], P('span', None, 'heads')
- stored_values: bfloat16 [4, 6144, 16, 128], P('span', None, 'heads')
The draws below stay inside these ranges and needn't reach their ends.
All inputs are finite; a program needn't handle non-finite values.
Results may differ from the reference program's by a relative error of at most 0.001.
Values may be sent and summed in bfloat16 or wider, within the bound.
A program may use at most 128 MiB of HBM per device.

```python
import jax
import jax.numpy as jnp
from jax import lax

BATCH = 4
LENGTH = 6144
HEADS = 16
LATENT = 512
KEY_PART = 128
ROTARY = 64
VALUE_SIZE = 128


def block_scale(own_key, shape, cuts, least, largest):
    def one(position, parts):
        steps = jax.random.uniform(jax.random.fold_in(jax.random.fold_in(own_key, 6), position), (parts,), jnp.float32, least / len(cuts), largest / len(cuts))
        return jnp.repeat(jnp.exp(steps), shape[position] // parts).reshape((-1,) + (1,) * (len(shape) - position - 1))

    factor_of = one(*cuts[0])
    for cut in cuts[1:]:
        factor_of = factor_of * one(*cut)
    return factor_of


def scatter_about(stream_key, dims, width, most, split=(), kind=jnp.bfloat16):
    result = jax.random.normal(stream_key, dims, jnp.float32) * width
    if len(split) > 0:
        result = block_scale(stream_key, dims, split, -0.22, 0.18) * result
    return jnp.clip(result, min=-most, max=most).astype(kind)


def setup_inputs(seed: int = 0) -> dict:
    key_list = jax.random.split(jax.random.key(seed), 6)
    latents = scatter_about(key_list[0], (BATCH, LENGTH, LATENT), 1.0, 6.0, ((1, 32),))
    rotary_rows = scatter_about(key_list[1], (BATCH, LENGTH, ROTARY), 1.0, 6.0, ((1, 32),))
    latent_gain = jnp.clip(1.0 + 0.15 * jax.random.normal(key_list[2], (LATENT,), jnp.float32), 0.25, 1.75)
    key_up = scatter_about(key_list[3], (LATENT, HEADS, KEY_PART), LATENT ** -0.5, 0.25, ((1, 8),))
    value_up = scatter_about(key_list[4], (LATENT, HEADS, VALUE_SIZE), LATENT ** -0.5, 0.25, ((1, 8),))
    return {"latents": latents, "rotary_rows": rotary_rows, "latent_gain": latent_gain, "key_up": key_up, "value_up": value_up}


def root_norm(vectors, row_gain):
    return vectors * lax.rsqrt(lax.optimization_barrier(jnp.mean(vectors * vectors, axis=-1, keepdims=True)) + 1e-06) * row_gain

def reference(latents, rotary_rows, latent_gain, key_up, value_up):
    rows_ready = root_norm(latents.astype(jnp.float32), latent_gain).astype(jnp.bfloat16)
    rows_ready = lax.optimization_barrier(rows_ready)

    def expand_one(one):
        rows_one, rotary_one = one
        wide_keys = jnp.einsum('tr,rhk->thk', rows_one.astype(jnp.float32), key_up.astype(jnp.float32)).astype(jnp.bfloat16)
        shared = jnp.broadcast_to(rotary_one[:, None], (LENGTH, HEADS, ROTARY))
        wide_values = jnp.einsum('tr,rhk->thk', rows_one.astype(jnp.float32), value_up.astype(jnp.float32)).astype(jnp.bfloat16)
        return (jnp.concatenate([wide_keys, shared], axis=-1), wide_values)
    stored_keys, stored_values = lax.map(expand_one, (rows_ready, rotary_rows))
    return (stored_keys, stored_values)
```

```python
import functools

import jax
import jax.numpy as jnp
from jax import lax
from jax.experimental import pallas as pl
from jax.experimental.pallas import tpu as pltpu
from jax.sharding import PartitionSpec as P

MESH = pl.DeviceIdType.MESH
PIECES = 2


def gather_kernel(sizes, rows_ref, rotary_ref, rows_out, rotary_out, *sems):
    spans, chips, cores, pieces = sizes
    recv_sem, plane_sem, up_sem, down_sem, partner_sem, own_sem = sems
    block = rows_ref.shape[1]
    cut = block // pieces
    me_s = lax.axis_index("span")
    me_h = lax.axis_index("heads")
    z, c = me_h // cores, me_h % cores

    def span_of(i):
        if spans & (spans - 1):
            return (me_s + i) % spans
        total, bit = 0, 1
        while bit < spans:
            total = total + ((me_s // bit + i // bit) % 2) * bit
            bit *= 2
        return total

    def to(span, heads):
        return {"span": span, "heads": heads}

    def mine(span, piece):
        if piece < pieces:
            return rows_ref.at[span, pl.ds(piece * cut, cut)]
        return rotary_ref.at[span]

    def slot(span, chip, core, piece):
        if piece < pieces:
            return rows_out.at[span, chip * cores + core, pl.ds(piece * cut, cut)]
        return rotary_out.at[span, chip * cores + core]

    def arrived(span, chip, core, piece):
        return recv_sem.at[span, chip * cores + core, piece]

    def push(src, span, chip, piece, send_sem, device):
        return pltpu.make_async_remote_copy(
            src_ref=src,
            dst_ref=slot(span, chip, c, piece),
            send_sem=send_sem,
            recv_sem=arrived(span, chip, c, piece),
            device_id=device,
            device_id_type=MESH,
        )

    def wait_block(span, chip, core, piece):
        ref = slot(span, chip, core, piece)
        pltpu.make_async_remote_copy(
            src_ref=ref,
            dst_ref=ref,
            send_sem=arrived(span, chip, core, piece),
            recv_sem=arrived(span, chip, core, piece),
            device_id=to(me_s, me_h),
            device_id_type=MESH,
        ).wait_recv()

    up = lambda src, span, chip, p: push(
        src, span, chip, p, up_sem.at[span, chip, p], to(me_s, me_h + cores)
    )
    down = lambda src, span, chip, p: push(
        src, span, chip, p, down_sem.at[span, chip, p], to(me_s, me_h - cores)
    )
    across = lambda src, span, chip, p: push(
        src, span, chip, p, partner_sem.at[span, chip, p], to(me_s, z * cores + (c + 1) % cores)
    )
    has_up, has_down = z < chips - 1, z > 0

    barrier = pltpu.get_barrier_semaphore()

    def greet(device):
        pl.semaphore_signal(barrier, inc=1, device_id=device, device_id_type=MESH)

    for i in range(1, spans):
        greet(to(span_of(i), me_h))
    if cores > 1:
        greet(to(me_s, z * cores + (c + 1) % cores))
    pl.when(has_up)(lambda: greet(to(me_s, me_h + cores)))
    pl.when(has_down)(lambda: greet(to(me_s, me_h - cores)))
    peers = spans - 1 + (cores > 1) + jnp.where(has_up, 1, 0) + jnp.where(has_down, 1, 0)
    pl.semaphore_wait(barrier, peers)

    parts = range(pieces + 1)

    def plane(i, p):
        return pltpu.make_async_remote_copy(
            src_ref=mine(span_of(i), p),
            dst_ref=slot(me_s, z, c, p),
            send_sem=plane_sem.at[i, p],
            recv_sem=arrived(me_s, z, c, p),
            device_id=to(span_of(i), me_h),
            device_id_type=MESH,
        )

    def own(p):
        return pltpu.make_async_copy(mine(me_s, p), slot(me_s, z, c, p), own_sem.at[p])

    for p in parts:
        pl.when(has_up)(lambda: up(mine(me_s, p), me_s, z, p).start())
        pl.when(has_down)(lambda: down(mine(me_s, p), me_s, z, p).start())
    for p in parts:
        for i in range(1, spans):
            plane(i, p).start()
    for p in parts:
        own(p).start()
        if cores > 1:
            across(mine(me_s, p), me_s, z, p).start()

    def first(i, _):
        span = span_of(i)
        for p in parts:
            wait_block(span, z, c, p)
            src = slot(span, z, c, p)
            pl.when(has_up)(lambda: up(src, span, z, p).start())
            pl.when(has_down)(lambda: down(src, span, z, p).start())
            if cores > 1:
                across(src, span, z, p).start()
        return 0

    lax.fori_loop(1, spans, first, 0)

    def later(step, _):
        r, span = step // spans, span_of(step % spans)

        def pass_on(chip, further, send):
            for p in parts:
                wait_block(span, chip, c, p)
                src = slot(span, chip, c, p)
                pl.when(further)(lambda: send(src, span, chip, p).start())
                if cores > 1:
                    across(src, span, chip, p).start()

        pl.when(z - r >= 0)(lambda: pass_on(z - r, has_up, up))
        pl.when(z + r < chips)(lambda: pass_on(z + r, has_down, down))
        return 0

    lax.fori_loop(spans, spans * chips, later, 0)

    for p in parts:
        own(p).wait()
        for i in range(1, spans):
            plane(i, p).wait_send()

    def finish(step, _):
        span, chip = step % spans, step // spans
        for p in parts:
            src = slot(span, chip, c, p)
            if cores > 1:
                across(src, span, chip, p).wait_send()
                wait_block(span, chip, (c + 1) % cores, p)
            pl.when(has_up & (chip <= z))(lambda: up(src, span, chip, p).wait_send())
            pl.when(has_down & (chip >= z))(lambda: down(src, span, chip, p).wait_send())
        return 0

    lax.fori_loop(0, spans * chips, finish, 0)


def gather(rows, rotary_t):
    spans, heads = lax.axis_size("span"), lax.axis_size("heads")
    cores = 2 if heads % 2 == 0 else 1
    chips = heads // cores
    block, width = rows.shape[1:]
    pieces = PIECES if block % (16 * PIECES) == 0 else 1
    parts = pieces + 1
    dma = pltpu.SemaphoreType.DMA
    return pl.pallas_call(
        functools.partial(gather_kernel, (spans, chips, cores, pieces)),
        out_shape=(
            OUT((spans, heads, block, width), rows.dtype),
            OUT((spans, heads) + rotary_t.shape[1:], rotary_t.dtype),
        ),
        in_specs=[pl.BlockSpec(memory_space=pl.ANY)] * 2,
        out_specs=[pl.BlockSpec(memory_space=OUT_SPACE)] * 2,
        scratch_shapes=[
            dma((spans, heads, parts)),
            dma((spans, parts)),
            dma((spans, chips, parts)),
            dma((spans, chips, parts)),
            dma((spans, chips, parts)),
            dma((parts,)),
        ],
        compiler_params=pltpu.CompilerParams(
            collective_id=0, has_side_effects=True, vmem_limit_bytes=4 << 20
        ),
        name="gather",
    )(rows, rotary_t)


OUT = pltpu.VMEM
OUT_SPACE = pltpu.VMEM


def expand_kernel(group, rows_ref, rotary_ref, gain_ref, key_ref, value_ref, keys_out, values_out, mix):
    tile = pl.program_id(0)
    rows = rows_ref[pl.ds(tile * group, group)]
    rows = rows.reshape(-1, rows.shape[-1]).astype(jnp.float32)
    scale = lax.rsqrt(jnp.mean(rows * rows, axis=-1, keepdims=True) + 1e-06)
    ready = (rows * scale * gain_ref[...]).astype(jnp.bfloat16)
    count = ready.shape[0]
    heads, key_part = keys_out.shape[0], key_ref.shape[0] // keys_out.shape[0]
    keys = lax.dot_general(
        key_ref[...], ready, (((1,), (1,)), ((), ())), preferred_element_type=jnp.float32
    ).astype(jnp.bfloat16)
    values = jnp.dot(ready, value_ref[...], preferred_element_type=jnp.float32)
    turned = jnp.concatenate([rotary_ref[tile * group + g] for g in range(group)], axis=-1)
    size = values.shape[-1] // heads
    for h in range(heads):
        keys_out[h, :key_part] = keys[h * key_part : (h + 1) * key_part]
        keys_out[h, key_part:] = turned
        mix[pl.ds(h, count, stride=heads)] = values[:, h * size : (h + 1) * size]
    values_out[...] = mix[...].astype(values_out.dtype)


def expand(rows, rotary_t, gain, key_up, value_up):
    blocks, block, width = rows.shape
    heads, key_part = key_up.shape[1:]
    size = value_up.shape[2]
    turn = rotary_t.shape[1]
    group = 1
    while blocks % (2 * group) == 0 and (block * group < 768 or block * group % 128):
        group *= 2
    count = block * group
    whole = pl.BlockSpec(memory_space=pltpu.VMEM)
    keys, values = pl.pallas_call(
        functools.partial(expand_kernel, group),
        grid=(blocks // group,),
        out_shape=(
            jax.ShapeDtypeStruct((heads, key_part + turn, blocks * block), rows.dtype),
            jax.ShapeDtypeStruct((blocks * block * heads, size), rows.dtype),
        ),
        in_specs=[whole] * 5,
        out_specs=(
            pl.BlockSpec((heads, key_part + turn, count), lambda t: (0, 0, t)),
            pl.BlockSpec((count * heads, size), lambda t: (t, 0)),
        ),
        scratch_shapes=[pltpu.VMEM((count * heads, size), jnp.float32)],
        compiler_params=pltpu.CompilerParams(vmem_limit_bytes=24 << 20),
        name="expand",
    )(
        rows,
        rotary_t,
        gain[None],
        key_up.reshape(width, heads * key_part).T,
        value_up.reshape(width, heads * size),
    )
    stored_keys = keys.transpose(2, 0, 1)[None]
    return stored_keys, values.reshape(1, blocks * block, heads, size)


def per_device(latents, rotary_rows, latent_gain, key_up, value_up):
    rows, rotary = gather(latents, rotary_rows.transpose(0, 2, 1))
    rows = rows.reshape((-1,) + rows.shape[2:])
    rotary = rotary.reshape((-1,) + rotary.shape[2:])
    return expand(rows, rotary, latent_gain, key_up, value_up)


def solution(mesh):
    in_specs = (
        P(None, ("span", "heads"), None),
        P(None, ("span", "heads"), None),
        P(),
        P(None, "heads", None),
        P(None, "heads", None),
    )
    out_specs = (P("span", None, "heads", None), P("span", None, "heads", None))
    return jax.shard_map(
        per_device, mesh=mesh, in_specs=in_specs, out_specs=out_specs, check_vma=False
    )
```

```python
import functools

import jax
import jax.numpy as jnp
from jax import lax
from jax.experimental import pallas as pl
from jax.experimental.pallas import tpu as pltpu
from jax.sharding import PartitionSpec as P

MESH = pl.DeviceIdType.MESH
PIECES = 2


def gather_kernel(sizes, rows_ref, rotary_ref, rows_out, rotary_out, *sems):
    spans, chips, cores, pieces = sizes
    recv_sem, plane_sem, up_sem, down_sem, partner_sem, own_sem = sems
    block = rows_ref.shape[1]
    cut = block // pieces
    me_s = lax.axis_index("span")
    me_h = lax.axis_index("heads")
    z, c = me_h // cores, me_h % cores

    def span_of(i):
        if spans & (spans - 1):
            return (me_s + i) % spans
        total, bit = 0, 1
        while bit < spans:
            total = total + ((me_s // bit + i // bit) % 2) * bit
            bit *= 2
        return total

    def to(span, heads):
        return {"span": span, "heads": heads}

    def mine(span, piece):
        if piece < pieces:
            return rows_ref.at[span, pl.ds(piece * cut, cut)]
        return rotary_ref.at[span]

    def slot(span, chip, core, piece):
        if piece < pieces:
            return rows_out.at[span, chip * cores + core, pl.ds(piece * cut, cut)]
        return rotary_out.at[span, chip * cores + core]

    def arrived(span, chip, core, piece):
        return recv_sem.at[span, chip * cores + core, piece]

    def push(src, span, chip, piece, send_sem, device):
        return pltpu.make_async_remote_copy(
            src_ref=src,
            dst_ref=slot(span, chip, c, piece),
            send_sem=send_sem,
            recv_sem=arrived(span, chip, c, piece),
            device_id=device,
            device_id_type=MESH,
        )

    def wait_block(span, chip, core, piece):
        ref = slot(span, chip, core, piece)
        pltpu.make_async_remote_copy(
            src_ref=ref,
            dst_ref=ref,
            send_sem=arrived(span, chip, core, piece),
            recv_sem=arrived(span, chip, core, piece),
            device_id=to(me_s, me_h),
            device_id_type=MESH,
        ).wait_recv()

    up = lambda src, span, chip, p: push(
        src, span, chip, p, up_sem.at[span, chip, p], to(me_s, me_h + cores)
    )
    down = lambda src, span, chip, p: push(
        src, span, chip, p, down_sem.at[span, chip, p], to(me_s, me_h - cores)
    )
    across = lambda src, span, chip, p: push(
        src, span, chip, p, partner_sem.at[span, chip, p], to(me_s, z * cores + (c + 1) % cores)
    )
    has_up, has_down = z < chips - 1, z > 0

    barrier = pltpu.get_barrier_semaphore()

    def greet(device):
        pl.semaphore_signal(barrier, inc=1, device_id=device, device_id_type=MESH)

    for i in range(1, spans):
        greet(to(span_of(i), me_h))
    if cores > 1:
        greet(to(me_s, z * cores + (c + 1) % cores))
    pl.when(has_up)(lambda: greet(to(me_s, me_h + cores)))
    pl.when(has_down)(lambda: greet(to(me_s, me_h - cores)))
    peers = spans - 1 + (cores > 1) + jnp.where(has_up, 1, 0) + jnp.where(has_down, 1, 0)
    pl.semaphore_wait(barrier, peers)

    parts = range(pieces + 1)

    def plane(i, p):
        return pltpu.make_async_remote_copy(
            src_ref=mine(span_of(i), p),
            dst_ref=slot(me_s, z, c, p),
            send_sem=plane_sem.at[i, p],
            recv_sem=arrived(me_s, z, c, p),
            device_id=to(span_of(i), me_h),
            device_id_type=MESH,
        )

    def own(p):
        return pltpu.make_async_copy(mine(me_s, p), slot(me_s, z, c, p), own_sem.at[p])

    for p in parts:
        pl.when(has_up)(lambda: up(mine(me_s, p), me_s, z, p).start())
        pl.when(has_down)(lambda: down(mine(me_s, p), me_s, z, p).start())
    for p in parts:
        for i in range(1, spans):
            plane(i, p).start()
    for p in parts:
        own(p).start()
        if cores > 1:
            across(mine(me_s, p), me_s, z, p).start()

    def first(i, _):
        span = span_of(i)
        for p in parts:
            wait_block(span, z, c, p)
            src = slot(span, z, c, p)
            pl.when(has_up)(lambda: up(src, span, z, p).start())
            pl.when(has_down)(lambda: down(src, span, z, p).start())
            if cores > 1:
                across(src, span, z, p).start()
        return 0

    lax.fori_loop(1, spans, first, 0)

    def later(step, _):
        r, span = step // spans, span_of(step % spans)

        def pass_on(chip, further, send):
            for p in parts:
                wait_block(span, chip, c, p)
                src = slot(span, chip, c, p)
                pl.when(further)(lambda: send(src, span, chip, p).start())
                if cores > 1:
                    across(src, span, chip, p).start()

        pl.when(z - r >= 0)(lambda: pass_on(z - r, has_up, up))
        pl.when(z + r < chips)(lambda: pass_on(z + r, has_down, down))
        return 0

    lax.fori_loop(spans, spans * chips, later, 0)

    for p in parts:
        own(p).wait()
        for i in range(1, spans):
            plane(i, p).wait_send()

    def finish(step, _):
        span, chip = step % spans, step // spans
        for p in parts:
            src = slot(span, chip, c, p)
            if cores > 1:
                across(src, span, chip, p).wait_send()
                wait_block(span, chip, (c + 1) % cores, p)
            pl.when(has_up & (chip <= z))(lambda: up(src, span, chip, p).wait_send())
            pl.when(has_down & (chip >= z))(lambda: down(src, span, chip, p).wait_send())
        return 0

    lax.fori_loop(0, spans * chips, finish, 0)


def gather(rows, rotary_t):
    spans, heads = lax.axis_size("span"), lax.axis_size("heads")
    cores = 2 if heads % 2 == 0 else 1
    chips = heads // cores
    block, width = rows.shape[1:]
    pieces = PIECES if block % (16 * PIECES) == 0 else 1
    parts = pieces + 1
    dma = pltpu.SemaphoreType.DMA
    return pl.pallas_call(
        functools.partial(gather_kernel, (spans, chips, cores, pieces)),
        out_shape=(
            OUT((spans, heads, block, width), rows.dtype),
            OUT((spans, heads) + rotary_t.shape[1:], rotary_t.dtype),
        ),
        in_specs=[pl.BlockSpec(memory_space=pl.ANY)] * 2,
        out_specs=[pl.BlockSpec(memory_space=OUT_SPACE)] * 2,
        scratch_shapes=[
            dma((spans, heads, parts)),
            dma((spans, parts)),
            dma((spans, chips, parts)),
            dma((spans, chips, parts)),
            dma((spans, chips, parts)),
            dma((parts,)),
        ],
        compiler_params=pltpu.CompilerParams(
            collective_id=0, has_side_effects=True, vmem_limit_bytes=4 << 20
        ),
        name="gather",
    )(rows, rotary_t)


OUT = pltpu.VMEM
OUT_SPACE = pltpu.VMEM


def expand_kernel(group, rows_ref, rotary_ref, gain_ref, key_ref, value_ref, keys_out, values_out, mix):
    tile = pl.program_id(0)
    rows = rows_ref[pl.ds(tile * group, group)]
    rows = rows.reshape(-1, rows.shape[-1]).astype(jnp.float32)
    scale = lax.rsqrt(jnp.mean(rows * rows, axis=-1, keepdims=True) + 1e-06)
    ready = (rows * scale * gain_ref[...]).astype(jnp.bfloat16)
    count = ready.shape[0]
    heads, key_part = keys_out.shape[0], key_ref.shape[0] // keys_out.shape[0]
    keys = lax.dot_general(
        key_ref[...], ready, (((1,), (1,)), ((), ())), preferred_element_type=jnp.float32
    ).astype(jnp.bfloat16)
    values = jnp.dot(ready, value_ref[...], preferred_element_type=jnp.float32)
    turned = jnp.concatenate([rotary_ref[tile * group + g] for g in range(group)], axis=-1)
    size = values.shape[-1] // heads
    for h in range(heads):
        keys_out[h, :key_part] = keys[h * key_part : (h + 1) * key_part]
        keys_out[h, key_part:] = turned
        mix[pl.ds(h, count, stride=heads)] = values[:, h * size : (h + 1) * size]
    values_out[...] = mix[...].astype(values_out.dtype)


def expand(rows, rotary_t, gain, key_up, value_up):
    blocks, block, width = rows.shape
    heads, key_part = key_up.shape[1:]
    size = value_up.shape[2]
    turn = rotary_t.shape[1]
    group = 1
    while blocks % (2 * group) == 0 and (block * group < 768 or block * group % 128):
        group *= 2
    count = block * group
    whole = pl.BlockSpec(memory_space=pltpu.VMEM)
    keys, values = pl.pallas_call(
        functools.partial(expand_kernel, group),
        grid=(blocks // group,),
        out_shape=(
            jax.ShapeDtypeStruct((heads, key_part + turn, blocks * block), rows.dtype),
            jax.ShapeDtypeStruct((blocks * block * heads, size), rows.dtype),
        ),
        in_specs=[whole] * 5,
        out_specs=(
            pl.BlockSpec((heads, key_part + turn, count), lambda t: (0, 0, t)),
            pl.BlockSpec((count * heads, size), lambda t: (t, 0)),
        ),
        scratch_shapes=[pltpu.VMEM((count * heads, size), jnp.float32)],
        compiler_params=pltpu.CompilerParams(vmem_limit_bytes=24 << 20),
        name="expand",
    )(
        rows,
        rotary_t,
        gain[None],
        key_up.reshape(width, heads * key_part).T,
        value_up.reshape(width, heads * size),
    )
    stored_keys = keys.transpose(2, 0, 1)[None]
    return stored_keys, values.reshape(1, blocks * block, heads, size)


def fused_kernel(
    sizes, rows_ref, rotary_ref, gain_ref, key_ref, value_ref, keys_out, values_out, *scratch
):
    spans, chips, cores, pieces, packed = sizes
    held, turned_held, rows_in, gain, key_in, value_in, wide, key_t, value_w, mix = scratch[:10]
    recv_sem, plane_sem, up_sem, down_sem, partner_sem, own_sem, load_sem = scratch[10:]
    block, width = rows_ref.shape[1:]
    cut = block // pieces
    me_s = lax.axis_index("span")
    me_h = lax.axis_index("heads")
    z, c = me_h // cores, me_h % cores
    other = (c + 1) % cores
    parts = range(pieces + 1)

    def span_of(i):
        if spans & (spans - 1):
            return (me_s + i) % spans
        total, bit = 0, 1
        while bit < spans:
            total = total + ((me_s // bit + i // bit) % 2) * bit
            bit *= 2
        return total

    def to(span, heads):
        return {"span": span, "heads": heads}

    def slot(span, chip, core, piece):
        if piece < pieces:
            return held.at[span, chip * cores + core, pl.ds(piece * cut, cut)]
        return turned_held.at[span, chip * cores + core]

    def mine(i, piece):
        if piece < pieces:
            return rows_in.at[span_of(i), pl.ds(piece * cut, cut)]
        return rotary_ref.at[span_of(i)]

    def arrived(span, chip, core, piece):
        return recv_sem.at[span, chip * cores + core, piece]

    def push(src, span, chip, piece, send_sem, device):
        return pltpu.make_async_remote_copy(
            src_ref=src,
            dst_ref=slot(span, chip, c, piece),
            send_sem=send_sem,
            recv_sem=arrived(span, chip, c, piece),
            device_id=device,
            device_id_type=MESH,
        )

    def wait_block(span, chip, core, piece):
        ref = slot(span, chip, core, piece)
        pltpu.make_async_remote_copy(
            src_ref=ref,
            dst_ref=ref,
            send_sem=arrived(span, chip, core, piece),
            recv_sem=arrived(span, chip, core, piece),
            device_id=to(me_s, me_h),
            device_id_type=MESH,
        ).wait_recv()

    def up(src, span, chip, p):
        return push(src, span, chip, p, up_sem.at[span, chip, p], to(me_s, me_h + cores))

    def down(src, span, chip, p):
        return push(src, span, chip, p, down_sem.at[span, chip, p], to(me_s, me_h - cores))

    def across(src, span, chip, p):
        device = to(me_s, z * cores + other)
        return push(src, span, chip, p, partner_sem.at[span, chip, p], device)

    def plane(i, p):
        device = to(span_of(i), me_h)
        return push(mine(i, p), me_s, z, p, plane_sem.at[i, p], device)

    has_up, has_down = z < chips - 1, z > 0

    loads = [
        pltpu.make_async_copy(rows_ref, rows_in, load_sem.at[0]),
        pltpu.make_async_copy(rows_ref.at[me_s], held.at[me_s, me_h], load_sem.at[1]),
        pltpu.make_async_copy(rotary_ref.at[me_s], turned_held.at[me_s, me_h], load_sem.at[2]),
        pltpu.make_async_copy(gain_ref, gain, load_sem.at[3]),
        pltpu.make_async_copy(key_ref, key_in, load_sem.at[4]),
        pltpu.make_async_copy(value_ref, value_in, load_sem.at[5]),
    ]
    for load in loads:
        load.start()

    barrier = pltpu.get_barrier_semaphore()

    def greet(device):
        pl.semaphore_signal(barrier, inc=1, device_id=device, device_id_type=MESH)

    for i in range(1, spans):
        greet(to(span_of(i), me_h))
    if cores > 1:
        greet(to(me_s, z * cores + other))
    pl.when(has_up)(lambda: greet(to(me_s, me_h + cores)))
    pl.when(has_down)(lambda: greet(to(me_s, me_h - cores)))
    loads[0].wait()
    peers = spans - 1 + (cores > 1) + jnp.where(has_up, 1, 0) + jnp.where(has_down, 1, 0)
    pl.semaphore_wait(barrier, peers)

    def spread(src, span, chip, p, upward, downward):
        pl.when(upward)(lambda: up(src, span, chip, p).start())
        pl.when(downward)(lambda: down(src, span, chip, p).start())
        if cores > 1:
            across(src, span, chip, p).start()

    for p in parts:
        spread(mine(0, p), me_s, z, p, has_up, has_down)
        for i in range(1, min(spans, 3)):
            plane(i, p).start()
    for i in range(3, spans):
        for p in parts:
            plane(i, p).start()

    for load in loads[1:]:
        load.wait()
    heads, turn = keys_out.shape[0], turned_rows(turned_held.shape[2:], block)
    key_part = keys_out.shape[1] - turn
    size = values_out.shape[1]
    wide[...] = key_in[...].astype(jnp.float32)
    for h in range(heads):
        key_t[h * key_part : (h + 1) * key_part] = (
            wide[pl.ds(h, width, stride=heads)].T.astype(key_t.dtype)
        )
    wide[...] = value_in[...].astype(jnp.float32)
    for h in range(heads):
        value_w[:, h * size : (h + 1) * size] = (
            wide[pl.ds(h, width, stride=heads)].astype(value_w.dtype)
        )

    def turned(span, head):
        rows = turned_held[span, head]
        if not packed:
            return rows
        tail = rows[turn:]
        last = jnp.concatenate([tail[:, : block % 128], tail[:, block % 128 :]], axis=0)
        return jnp.concatenate([rows[:turn], last], axis=-1)

    count = block * cores

    def compute(span, chip):
        if cores > 1:
            for p in parts:
                wait_block(span, chip, other, p)
        first = chip * cores
        rows = held[span, pl.ds(first, cores)].reshape(count, width).astype(jnp.float32)
        scale = lax.rsqrt(jnp.mean(rows * rows, axis=-1, keepdims=True) + 1e-06)
        ready = (rows * scale * gain[...]).astype(jnp.bfloat16)
        keys = lax.dot_general(
            key_t[...], ready, (((1,), (1,)), ((), ())), preferred_element_type=jnp.float32
        ).astype(keys_out.dtype)
        values = jnp.dot(ready, value_w[...], preferred_element_type=jnp.float32)
        shared = jnp.concatenate([turned(span, first + k) for k in range(cores)], axis=-1)
        unit = span * chips + chip
        places = pl.ds(pl.multiple_of(unit * count, 128), count)
        for h in range(heads):
            keys_out[h, :key_part, places] = keys[h * key_part : (h + 1) * key_part]
            keys_out[h, key_part:, places] = shared
            mix[pl.ds(h, count, stride=heads)] = values[:, h * size : (h + 1) * size]
        lines = pl.ds(pl.multiple_of(unit * count * heads, 128), count * heads)
        values_out[lines] = mix[...].astype(values_out.dtype)

    def first_step(i, _):
        span = span_of(i)
        for p in parts:
            wait_block(span, z, c, p)
            spread(slot(span, z, c, p), span, z, p, has_up, has_down)
        compute(span_of(i - 1), z)
        return 0

    lax.fori_loop(1, spans, first_step, 0)

    def later_step(step, _):
        def forward():
            r, span = step // spans, span_of(step % spans)

            def pass_on(chip, upward, downward):
                for p in parts:
                    wait_block(span, chip, c, p)
                    spread(slot(span, chip, c, p), span, chip, p, upward, downward)

            pl.when(z - r >= 0)(lambda: pass_on(z - r, has_up, False))
            pl.when(z + r < chips)(lambda: pass_on(z + r, False, has_down))

        pl.when(step < spans * chips)(forward)
        before = step - 1
        r, span = before // spans, span_of(before % spans)
        pl.when(z - r >= 0)(lambda: compute(span, z - r))
        pl.when((r > 0) & (z + r < chips))(lambda: compute(span, z + r))
        return 0

    lax.fori_loop(spans, spans * chips + 1, later_step, 0)

    for p in parts:
        for i in range(1, spans):
            plane(i, p).wait_send()

    def finish(step, _):
        span, chip = step % spans, step // spans
        for p in parts:
            src = slot(span, chip, c, p)
            if cores > 1:
                across(src, span, chip, p).wait_send()
            pl.when(has_up & (chip <= z))(lambda: up(src, span, chip, p).wait_send())
            pl.when(has_down & (chip >= z))(lambda: down(src, span, chip, p).wait_send())
        return 0

    lax.fori_loop(0, spans * chips, finish, 0)


def turned_rows(shape, block):
    return shape[0] * shape[1] // block


def fused(rows, rotary, gain, key_up, value_up, cores):
    spans, heads = lax.axis_size("span"), lax.axis_size("heads")
    chips = heads // cores
    batch, block, width = rows.shape
    mine, key_part = key_up.shape[1:]
    size = value_up.shape[2]
    turn = rotary.shape[2]
    rotary = rotary.transpose(0, 2, 1)
    packed = block == 192 and turn % 32 == 0
    if packed:
        full = block - block % 128
        tail = jnp.concatenate(
            [rotary[:, : turn // 2, full:], rotary[:, turn // 2 :, full:]], axis=2
        )
        rotary = jnp.concatenate(
            [rotary[:, :, k : k + 128] for k in range(0, full, 128)] + [tail], axis=1
        )
    pieces = PIECES if block % (16 * PIECES) == 0 else 1
    parts = pieces + 1
    total = spans * heads * block
    dma = pltpu.SemaphoreType.DMA
    hbm = pl.BlockSpec(memory_space=pltpu.HBM)
    vmem = pl.BlockSpec(memory_space=pltpu.VMEM)
    bf16, f32 = rows.dtype, jnp.float32
    beside = 2 * total * mine * (key_part + turn + size) + 2 * rotary.size
    grant = (67043328 - beside - (64 << 10)) // 4096 * 4096
    keys, values = pl.pallas_call(
        functools.partial(fused_kernel, (spans, chips, cores, pieces, packed)),
        out_shape=(
            pltpu.VMEM((mine, key_part + turn, total), bf16),
            pltpu.VMEM((total * mine, size), bf16),
        ),
        in_specs=[hbm, vmem, hbm, hbm, hbm],
        out_specs=[vmem] * 2,
        scratch_shapes=[
            pltpu.VMEM((spans, heads, block, width), bf16),
            pltpu.VMEM((spans, heads) + rotary.shape[1:], bf16),
            pltpu.VMEM(rows.shape, bf16),
            pltpu.VMEM((1, width), f32),
            pltpu.VMEM((width * mine, key_part), bf16),
            pltpu.VMEM((width * mine, size), bf16),
            pltpu.VMEM((width * mine, max(key_part, size)), f32),
            pltpu.VMEM((mine * key_part, width), bf16),
            pltpu.VMEM((width, mine * size), bf16),
            pltpu.VMEM((block * cores * mine, size), f32),
            dma((spans, heads, parts)),
            dma((spans, parts)),
            dma((spans, chips, parts)),
            dma((spans, chips, parts)),
            dma((spans, chips, parts)),
            dma((parts,)),
            dma((6,)),
        ],
        compiler_params=pltpu.CompilerParams(
            collective_id=0, has_side_effects=True, vmem_limit_bytes=grant
        ),
        name="fused",
    )(
        rows,
        rotary,
        gain[None],
        key_up.reshape(width * mine, key_part),
        value_up.reshape(width * mine, size),
    )
    stored_keys = keys.transpose(2, 0, 1)[None]
    return stored_keys, values.reshape(1, total, mine, size)


def per_device(latents, rotary_rows, latent_gain, key_up, value_up):
    cores = 2 if lax.axis_size("heads") % 2 == 0 else 1
    if latents.shape[1] * cores % 128 == 0 and key_up.shape[2] == value_up.shape[2]:
        return fused(latents, rotary_rows, latent_gain, key_up, value_up, cores)
    rows, rotary = gather(latents, rotary_rows.transpose(0, 2, 1))
    rows = rows.reshape((-1,) + rows.shape[2:])
    rotary = rotary.reshape((-1,) + rotary.shape[2:])
    return expand(rows, rotary, latent_gain, key_up, value_up)


def solution(mesh):
    in_specs = (
        P(None, ("span", "heads"), None),
        P(None, ("span", "heads"), None),
        P(),
        P(None, "heads", None),
        P(None, "heads", None),
    )
    out_specs = (P("span", None, "heads", None), P("span", None, "heads", None))
    return jax.shard_map(
        per_device, mesh=mesh, in_specs=in_specs, out_specs=out_specs, check_vma=False
    )
```

```python
import functools

import jax
import jax.numpy as jnp
from jax import lax
from jax.experimental import pallas as pl
from jax.experimental.pallas import tpu as pltpu
from jax.sharding import PartitionSpec as P

MESH = pl.DeviceIdType.MESH
PIECES = 2
OUT_PIECES = 4


def gather_kernel(sizes, rows_ref, rotary_ref, rows_out, rotary_out, *sems):
    spans, chips, cores, pieces = sizes
    recv_sem, plane_sem, up_sem, down_sem, partner_sem, own_sem = sems
    block = rows_ref.shape[1]
    cut = block // pieces
    me_s = lax.axis_index("span")
    me_h = lax.axis_index("heads")
    z, c = me_h // cores, me_h % cores

    def span_of(i):
        if spans & (spans - 1):
            return (me_s + i) % spans
        total, bit = 0, 1
        while bit < spans:
            total = total + ((me_s // bit + i // bit) % 2) * bit
            bit *= 2
        return total

    def to(span, heads):
        return {"span": span, "heads": heads}

    def mine(span, piece):
        if piece < pieces:
            return rows_ref.at[span, pl.ds(piece * cut, cut)]
        return rotary_ref.at[span]

    def slot(span, chip, core, piece):
        if piece < pieces:
            return rows_out.at[span, chip * cores + core, pl.ds(piece * cut, cut)]
        return rotary_out.at[span, chip * cores + core]

    def arrived(span, chip, core, piece):
        return recv_sem.at[span, chip * cores + core, piece]

    def push(src, span, chip, piece, send_sem, device):
        return pltpu.make_async_remote_copy(
            src_ref=src,
            dst_ref=slot(span, chip, c, piece),
            send_sem=send_sem,
            recv_sem=arrived(span, chip, c, piece),
            device_id=device,
            device_id_type=MESH,
        )

    def wait_block(span, chip, core, piece):
        ref = slot(span, chip, core, piece)
        pltpu.make_async_remote_copy(
            src_ref=ref,
            dst_ref=ref,
            send_sem=arrived(span, chip, core, piece),
            recv_sem=arrived(span, chip, core, piece),
            device_id=to(me_s, me_h),
            device_id_type=MESH,
        ).wait_recv()

    up = lambda src, span, chip, p: push(
        src, span, chip, p, up_sem.at[span, chip, p], to(me_s, me_h + cores)
    )
    down = lambda src, span, chip, p: push(
        src, span, chip, p, down_sem.at[span, chip, p], to(me_s, me_h - cores)
    )
    across = lambda src, span, chip, p: push(
        src, span, chip, p, partner_sem.at[span, chip, p], to(me_s, z * cores + (c + 1) % cores)
    )
    has_up, has_down = z < chips - 1, z > 0

    barrier = pltpu.get_barrier_semaphore()

    def greet(device):
        pl.semaphore_signal(barrier, inc=1, device_id=device, device_id_type=MESH)

    for i in range(1, spans):
        greet(to(span_of(i), me_h))
    if cores > 1:
        greet(to(me_s, z * cores + (c + 1) % cores))
    pl.when(has_up)(lambda: greet(to(me_s, me_h + cores)))
    pl.when(has_down)(lambda: greet(to(me_s, me_h - cores)))
    peers = spans - 1 + (cores > 1) + jnp.where(has_up, 1, 0) + jnp.where(has_down, 1, 0)
    pl.semaphore_wait(barrier, peers)

    parts = range(pieces + 1)

    def plane(i, p):
        return pltpu.make_async_remote_copy(
            src_ref=mine(span_of(i), p),
            dst_ref=slot(me_s, z, c, p),
            send_sem=plane_sem.at[i, p],
            recv_sem=arrived(me_s, z, c, p),
            device_id=to(span_of(i), me_h),
            device_id_type=MESH,
        )

    def own(p):
        return pltpu.make_async_copy(mine(me_s, p), slot(me_s, z, c, p), own_sem.at[p])

    for p in parts:
        pl.when(has_up)(lambda: up(mine(me_s, p), me_s, z, p).start())
        pl.when(has_down)(lambda: down(mine(me_s, p), me_s, z, p).start())
    for p in parts:
        for i in range(1, spans):
            plane(i, p).start()
    for p in parts:
        own(p).start()
        if cores > 1:
            across(mine(me_s, p), me_s, z, p).start()

    def first(i, _):
        span = span_of(i)
        for p in parts:
            wait_block(span, z, c, p)
            src = slot(span, z, c, p)
            pl.when(has_up)(lambda: up(src, span, z, p).start())
            pl.when(has_down)(lambda: down(src, span, z, p).start())
            if cores > 1:
                across(src, span, z, p).start()
        return 0

    lax.fori_loop(1, spans, first, 0)

    def later(step, _):
        r, span = step // spans, span_of(step % spans)

        def pass_on(chip, further, send):
            for p in parts:
                wait_block(span, chip, c, p)
                src = slot(span, chip, c, p)
                pl.when(further)(lambda: send(src, span, chip, p).start())
                if cores > 1:
                    across(src, span, chip, p).start()

        pl.when(z - r >= 0)(lambda: pass_on(z - r, has_up, up))
        pl.when(z + r < chips)(lambda: pass_on(z + r, has_down, down))
        return 0

    lax.fori_loop(spans, spans * chips, later, 0)

    for p in parts:
        own(p).wait()
        for i in range(1, spans):
            plane(i, p).wait_send()

    def finish(step, _):
        span, chip = step % spans, step // spans
        for p in parts:
            src = slot(span, chip, c, p)
            if cores > 1:
                across(src, span, chip, p).wait_send()
                wait_block(span, chip, (c + 1) % cores, p)
            pl.when(has_up & (chip <= z))(lambda: up(src, span, chip, p).wait_send())
            pl.when(has_down & (chip >= z))(lambda: down(src, span, chip, p).wait_send())
        return 0

    lax.fori_loop(0, spans * chips, finish, 0)


def gather(rows, rotary_t):
    spans, heads = lax.axis_size("span"), lax.axis_size("heads")
    cores = 2 if heads % 2 == 0 else 1
    chips = heads // cores
    block, width = rows.shape[1:]
    pieces = PIECES if block % (16 * PIECES) == 0 else 1
    parts = pieces + 1
    dma = pltpu.SemaphoreType.DMA
    return pl.pallas_call(
        functools.partial(gather_kernel, (spans, chips, cores, pieces)),
        out_shape=(
            OUT((spans, heads, block, width), rows.dtype),
            OUT((spans, heads) + rotary_t.shape[1:], rotary_t.dtype),
        ),
        in_specs=[pl.BlockSpec(memory_space=pl.ANY)] * 2,
        out_specs=[pl.BlockSpec(memory_space=OUT_SPACE)] * 2,
        scratch_shapes=[
            dma((spans, heads, parts)),
            dma((spans, parts)),
            dma((spans, chips, parts)),
            dma((spans, chips, parts)),
            dma((spans, chips, parts)),
            dma((parts,)),
        ],
        compiler_params=pltpu.CompilerParams(
            collective_id=0, has_side_effects=True, vmem_limit_bytes=4 << 20
        ),
        name="gather",
    )(rows, rotary_t)


OUT = pltpu.VMEM
OUT_SPACE = pltpu.VMEM


def expand_kernel(group, rows_ref, rotary_ref, gain_ref, key_ref, value_ref, keys_out, values_out, mix):
    tile = pl.program_id(0)
    rows = rows_ref[pl.ds(tile * group, group)]
    rows = rows.reshape(-1, rows.shape[-1]).astype(jnp.float32)
    scale = lax.rsqrt(jnp.mean(rows * rows, axis=-1, keepdims=True) + 1e-06)
    ready = (rows * scale * gain_ref[...]).astype(jnp.bfloat16)
    count = ready.shape[0]
    heads, key_part = keys_out.shape[0], key_ref.shape[0] // keys_out.shape[0]
    keys = lax.dot_general(
        key_ref[...], ready, (((1,), (1,)), ((), ())), preferred_element_type=jnp.float32
    ).astype(jnp.bfloat16)
    values = jnp.dot(ready, value_ref[...], preferred_element_type=jnp.float32)
    turned = jnp.concatenate([rotary_ref[tile * group + g] for g in range(group)], axis=-1)
    size = values.shape[-1] // heads
    for h in range(heads):
        keys_out[h, :key_part] = keys[h * key_part : (h + 1) * key_part]
        keys_out[h, key_part:] = turned
        mix[pl.ds(h, count, stride=heads)] = values[:, h * size : (h + 1) * size]
    values_out[...] = mix[...].astype(values_out.dtype)


def expand(rows, rotary_t, gain, key_up, value_up):
    blocks, block, width = rows.shape
    heads, key_part = key_up.shape[1:]
    size = value_up.shape[2]
    turn = rotary_t.shape[1]
    group = 1
    while blocks % (2 * group) == 0 and (block * group < 768 or block * group % 128):
        group *= 2
    count = block * group
    whole = pl.BlockSpec(memory_space=pltpu.VMEM)
    keys, values = pl.pallas_call(
        functools.partial(expand_kernel, group),
        grid=(blocks // group,),
        out_shape=(
            jax.ShapeDtypeStruct((heads, key_part + turn, blocks * block), rows.dtype),
            jax.ShapeDtypeStruct((blocks * block * heads, size), rows.dtype),
        ),
        in_specs=[whole] * 5,
        out_specs=(
            pl.BlockSpec((heads, key_part + turn, count), lambda t: (0, 0, t)),
            pl.BlockSpec((count * heads, size), lambda t: (t, 0)),
        ),
        scratch_shapes=[pltpu.VMEM((count * heads, size), jnp.float32)],
        compiler_params=pltpu.CompilerParams(vmem_limit_bytes=24 << 20),
        name="expand",
    )(
        rows,
        rotary_t,
        gain[None],
        key_up.reshape(width, heads * key_part).T,
        value_up.reshape(width, heads * size),
    )
    stored_keys = keys.transpose(2, 0, 1)[None]
    return stored_keys, values.reshape(1, blocks * block, heads, size)


def fused_kernel(
    sizes, rows_ref, rotary_ref, gain_ref, key_ref, value_ref, keys_out, values_out, *scratch
):
    spans, chips, cores, pieces, packed = sizes
    held, turned_held, rows_in, gain, key_in, value_in, wide, key_t, value_w, mix = scratch[:10]
    recv_sem, plane_sem, up_sem, down_sem, partner_sem, own_sem, load_sem = scratch[10:]
    block, width = rows_ref.shape[1:]
    cut = block // pieces
    me_s = lax.axis_index("span")
    me_h = lax.axis_index("heads")
    z, c = me_h // cores, me_h % cores
    other = (c + 1) % cores
    parts = range(pieces + 1)

    def span_of(i):
        if spans & (spans - 1):
            return (me_s + i) % spans
        total, bit = 0, 1
        while bit < spans:
            total = total + ((me_s // bit + i // bit) % 2) * bit
            bit *= 2
        return total

    def to(span, heads):
        return {"span": span, "heads": heads}

    def slot(span, chip, core, piece):
        if piece < pieces:
            return held.at[span, chip * cores + core, pl.ds(piece * cut, cut)]
        return turned_held.at[span, chip * cores + core]

    def mine(i, piece):
        if piece < pieces:
            return rows_in.at[span_of(i), pl.ds(piece * cut, cut)]
        return rotary_ref.at[span_of(i)]

    def arrived(span, chip, core, piece):
        return recv_sem.at[span, chip * cores + core, piece]

    def push(src, span, chip, piece, send_sem, device):
        return pltpu.make_async_remote_copy(
            src_ref=src,
            dst_ref=slot(span, chip, c, piece),
            send_sem=send_sem,
            recv_sem=arrived(span, chip, c, piece),
            device_id=device,
            device_id_type=MESH,
        )

    def wait_block(span, chip, core, piece):
        ref = slot(span, chip, core, piece)
        pltpu.make_async_remote_copy(
            src_ref=ref,
            dst_ref=ref,
            send_sem=arrived(span, chip, core, piece),
            recv_sem=arrived(span, chip, core, piece),
            device_id=to(me_s, me_h),
            device_id_type=MESH,
        ).wait_recv()

    def up(src, span, chip, p):
        return push(src, span, chip, p, up_sem.at[span, chip, p], to(me_s, me_h + cores))

    def down(src, span, chip, p):
        return push(src, span, chip, p, down_sem.at[span, chip, p], to(me_s, me_h - cores))

    def across(src, span, chip, p):
        device = to(me_s, z * cores + other)
        return push(src, span, chip, p, partner_sem.at[span, chip, p], device)

    def plane(i, p):
        device = to(span_of(i), me_h)
        return push(mine(i, p), me_s, z, p, plane_sem.at[i, p], device)

    has_up, has_down = z < chips - 1, z > 0

    loads = [
        pltpu.make_async_copy(rows_ref, rows_in, load_sem.at[0]),
        pltpu.make_async_copy(rows_ref.at[me_s], held.at[me_s, me_h], load_sem.at[1]),
        pltpu.make_async_copy(rotary_ref.at[me_s], turned_held.at[me_s, me_h], load_sem.at[2]),
        pltpu.make_async_copy(gain_ref, gain, load_sem.at[3]),
        pltpu.make_async_copy(key_ref, key_in, load_sem.at[4]),
        pltpu.make_async_copy(value_ref, value_in, load_sem.at[5]),
    ]
    for load in loads:
        load.start()

    barrier = pltpu.get_barrier_semaphore()

    def greet(device):
        pl.semaphore_signal(barrier, inc=1, device_id=device, device_id_type=MESH)

    for i in range(1, spans):
        greet(to(span_of(i), me_h))
    if cores > 1:
        greet(to(me_s, z * cores + other))
    pl.when(has_up)(lambda: greet(to(me_s, me_h + cores)))
    pl.when(has_down)(lambda: greet(to(me_s, me_h - cores)))
    loads[0].wait()
    peers = spans - 1 + (cores > 1) + jnp.where(has_up, 1, 0) + jnp.where(has_down, 1, 0)
    pl.semaphore_wait(barrier, peers)

    def spread(src, span, chip, p, upward, downward):
        pl.when(upward)(lambda: up(src, span, chip, p).start())
        pl.when(downward)(lambda: down(src, span, chip, p).start())
        if cores > 1:
            across(src, span, chip, p).start()

    for p in parts:
        spread(mine(0, p), me_s, z, p, has_up, has_down)
        for i in range(1, min(spans, 3)):
            plane(i, p).start()
    for i in range(3, spans):
        for p in parts:
            plane(i, p).start()

    for load in loads[1:]:
        load.wait()
    heads, turn = keys_out.shape[0], turned_rows(turned_held.shape[2:], block)
    key_part = keys_out.shape[1] - turn
    size = values_out.shape[1]
    wide[...] = key_in[...].astype(jnp.float32)
    for h in range(heads):
        key_t[h * key_part : (h + 1) * key_part] = (
            wide[pl.ds(h, width, stride=heads)].T.astype(key_t.dtype)
        )
    wide[...] = value_in[...].astype(jnp.float32)
    for h in range(heads):
        value_w[:, h * size : (h + 1) * size] = (
            wide[pl.ds(h, width, stride=heads)].astype(value_w.dtype)
        )

    def turned(span, head):
        rows = turned_held[span, head]
        if not packed:
            return rows
        tail = rows[turn:]
        last = jnp.concatenate([tail[:, : block % 128], tail[:, block % 128 :]], axis=0)
        return jnp.concatenate([rows[:turn], last], axis=-1)

    count = block * cores

    def compute(span, chip):
        if cores > 1:
            for p in parts:
                wait_block(span, chip, other, p)
        first = chip * cores
        rows = held[span, pl.ds(first, cores)].reshape(count, width).astype(jnp.float32)
        scale = lax.rsqrt(jnp.mean(rows * rows, axis=-1, keepdims=True) + 1e-06)
        ready = (rows * scale * gain[...]).astype(jnp.bfloat16)
        keys = lax.dot_general(
            key_t[...], ready, (((1,), (1,)), ((), ())), preferred_element_type=jnp.float32
        ).astype(keys_out.dtype)
        values = jnp.dot(ready, value_w[...], preferred_element_type=jnp.float32)
        shared = jnp.concatenate([turned(span, first + k) for k in range(cores)], axis=-1)
        unit = span * chips + chip
        places = pl.ds(pl.multiple_of(unit * count, 128), count)
        for h in range(heads):
            keys_out[h, :key_part, places] = keys[h * key_part : (h + 1) * key_part]
            keys_out[h, key_part:, places] = shared
            mix[pl.ds(h, count, stride=heads)] = values[:, h * size : (h + 1) * size]
        lines = pl.ds(pl.multiple_of(unit * count * heads, 128), count * heads)
        values_out[lines] = mix[...].astype(values_out.dtype)

    def first_step(i, _):
        span = span_of(i)
        for p in parts:
            wait_block(span, z, c, p)
            spread(slot(span, z, c, p), span, z, p, has_up, has_down)
        compute(span_of(i - 1), z)
        return 0

    lax.fori_loop(1, spans, first_step, 0)

    def later_step(step, _):
        def forward():
            r, span = step // spans, span_of(step % spans)

            def pass_on(chip, upward, downward):
                for p in parts:
                    wait_block(span, chip, c, p)
                    spread(slot(span, chip, c, p), span, chip, p, upward, downward)

            pl.when(z - r >= 0)(lambda: pass_on(z - r, has_up, False))
            pl.when(z + r < chips)(lambda: pass_on(z + r, False, has_down))

        before = step - 1
        r, span = before // spans, span_of(before % spans)
        pl.when(z - r >= 0)(lambda: compute(span, z - r))
        pl.when((r > 0) & (z + r < chips))(lambda: compute(span, z + r))
        pl.when(step < spans * chips)(forward)
        return 0

    lax.fori_loop(spans, spans * chips + 1, later_step, 0)

    for p in parts:
        for i in range(1, spans):
            plane(i, p).wait_send()

    def finish(step, _):
        span, chip = step % spans, step // spans
        for p in parts:
            src = slot(span, chip, c, p)
            if cores > 1:
                across(src, span, chip, p).wait_send()
            pl.when(has_up & (chip <= z))(lambda: up(src, span, chip, p).wait_send())
            pl.when(has_down & (chip >= z))(lambda: down(src, span, chip, p).wait_send())
        return 0

    lax.fori_loop(0, spans * chips, finish, 0)


def pack_kernel(turn, rows_ref, packed_ref):
    half, full = turn // 2, packed_ref.shape[2]
    rest = full // 2
    for b in range(rows_ref.shape[0]):
        packed_ref[b, :turn] = rows_ref[b, :, :full]
        packed_ref[b, turn:, :rest] = rows_ref[b, :half, full:]
        packed_ref[b, turn:, rest:] = rows_ref[b, half:, full:]


def pack(rotary, block):
    batch, turn = rotary.shape[:2]
    vmem = pl.BlockSpec(memory_space=pltpu.VMEM)
    return pl.pallas_call(
        functools.partial(pack_kernel, turn),
        out_shape=pltpu.VMEM((batch, turn * block // 128, 128), rotary.dtype),
        in_specs=[vmem],
        out_specs=vmem,
        compiler_params=pltpu.CompilerParams(vmem_limit_bytes=4 << 20),
        name="pack",
    )(rotary)


def copy_out_kernel(pieces, keys_ref, values_ref, keys_out, values_out, sem):
    copies = []
    for src, dst in ((keys_ref, keys_out), (values_ref, values_out)):
        step = src.shape[-2] // pieces
        for k in range(pieces):
            for h in range(src.shape[0] if len(src.shape) == 3 else 1):
                rows = pl.ds(k * step, step)
                at = (h, rows) if len(src.shape) == 3 else (rows,)
                copies.append(
                    pltpu.make_async_copy(src.at[at], dst.at[at], sem.at[len(copies)])
                )
    for copy in copies:
        copy.start()
    for copy in copies:
        copy.wait()


def copy_out(keys, values):
    pieces = OUT_PIECES
    vmem = pl.BlockSpec(memory_space=pltpu.VMEM)
    hbm = pl.BlockSpec(memory_space=pltpu.HBM)
    return pl.pallas_call(
        functools.partial(copy_out_kernel, pieces),
        out_shape=[jax.ShapeDtypeStruct(x.shape, x.dtype) for x in (keys, values)],
        in_specs=[vmem] * 2,
        out_specs=[hbm] * 2,
        scratch_shapes=[pltpu.SemaphoreType.DMA((pieces * (keys.shape[0] + 1),))],
        compiler_params=pltpu.CompilerParams(vmem_limit_bytes=1 << 20),
        name="copy_out",
    )(keys, values)


def turned_rows(shape, block):
    return shape[0] * shape[1] // block


def fused(rows, rotary, gain, key_up, value_up, cores):
    spans, heads = lax.axis_size("span"), lax.axis_size("heads")
    chips = heads // cores
    batch, block, width = rows.shape
    mine, key_part = key_up.shape[1:]
    size = value_up.shape[2]
    turn = rotary.shape[2]
    rotary = rotary.transpose(0, 2, 1)
    packed = block == 192 and turn % 32 == 0
    if packed:
        rotary = pltpu.with_memory_space_constraint(pack(rotary, block), pltpu.VMEM)
    pieces = PIECES if block % (16 * PIECES) == 0 else 1
    parts = pieces + 1
    total = spans * heads * block
    dma = pltpu.SemaphoreType.DMA
    hbm = pl.BlockSpec(memory_space=pltpu.HBM)
    vmem = pl.BlockSpec(memory_space=pltpu.VMEM)
    bf16, f32 = rows.dtype, jnp.float32
    beside = 2 * total * mine * (key_part + turn + size) + 2 * rotary.size
    grant = (67043328 - beside - (224 << 10)) // 4096 * 4096
    keys, values = pl.pallas_call(
        functools.partial(fused_kernel, (spans, chips, cores, pieces, packed)),
        out_shape=(
            pltpu.VMEM((mine, key_part + turn, total), bf16),
            pltpu.VMEM((total * mine, size), bf16),
        ),
        in_specs=[hbm, vmem, hbm, hbm, hbm],
        out_specs=[vmem] * 2,
        scratch_shapes=[
            pltpu.VMEM((spans, heads, block, width), bf16),
            pltpu.VMEM((spans, heads) + rotary.shape[1:], bf16),
            pltpu.VMEM(rows.shape, bf16),
            pltpu.VMEM((1, width), f32),
            pltpu.VMEM((width * mine, key_part), bf16),
            pltpu.VMEM((width * mine, size), bf16),
            pltpu.VMEM((width * mine, max(key_part, size)), f32),
            pltpu.VMEM((mine * key_part, width), bf16),
            pltpu.VMEM((width, mine * size), bf16),
            pltpu.VMEM((block * cores * mine, size), f32),
            dma((spans, heads, parts)),
            dma((spans, parts)),
            dma((spans, chips, parts)),
            dma((spans, chips, parts)),
            dma((spans, chips, parts)),
            dma((parts,)),
            dma((6,)),
        ],
        compiler_params=pltpu.CompilerParams(
            collective_id=0, has_side_effects=True, vmem_limit_bytes=grant
        ),
        name="fused",
    )(
        rows,
        rotary,
        gain[None],
        key_up.reshape(width * mine, key_part),
        value_up.reshape(width * mine, size),
    )
    keys, values = copy_out(keys, values)
    stored_keys = keys.transpose(2, 0, 1)[None]
    return stored_keys, values.reshape(1, total, mine, size)


def per_device(latents, rotary_rows, latent_gain, key_up, value_up):
    cores = 2 if lax.axis_size("heads") % 2 == 0 else 1
    if latents.shape[1] * cores % 128 == 0 and key_up.shape[2] == value_up.shape[2]:
        return fused(latents, rotary_rows, latent_gain, key_up, value_up, cores)
    rows, rotary = gather(latents, rotary_rows.transpose(0, 2, 1))
    rows = rows.reshape((-1,) + rows.shape[2:])
    rotary = rotary.reshape((-1,) + rotary.shape[2:])
    return expand(rows, rotary, latent_gain, key_up, value_up)


def solution(mesh):
    in_specs = (
        P(None, ("span", "heads"), None),
        P(None, ("span", "heads"), None),
        P(),
        P(None, "heads", None),
        P(None, "heads", None),
    )
    out_specs = (P("span", None, "heads", None), P("span", None, "heads", None))
    return jax.shard_map(
        per_device, mesh=mesh, in_specs=in_specs, out_specs=out_specs, check_vma=False
    )
```
